32 devices in a mesh: tm: 4 (over y, x), space: 8 (over z, core).
Axes of the slice: x: 2, y: 2, z: 4, core: 2. Of those that a mesh axis runs over, the one named last changes fastest.
Arguments:
- positions: float32 [4, 3, 3, 2048], P('tm', None, None, 'space'), may hold values from -4 to 4
- velocities: float32 [4, 3, 3, 2048], P('tm', None, None, 'space'), may hold values from -3 to 3
- masses: float32 [2048], P('space'), may hold values from 0.2 to 2
- initial_places: float32 [3, 2048], P(None, 'space'), may hold values from -4 to 4
- initial_speeds: float32 [3, 2048], P(None, 'space'), may hold values from -3 to 3
Outputs:
- node_places: float32 [4, 2, 3, 2048], P('tm', None, None, 'space')
- node_speeds: float32 [4, 2, 3, 2048], P('tm', None, None, 'space')
- end_force: float32 [4, 3, 2048], P('tm', None, 'space')
- start_places: float32 [4, 3, 2048], P('tm', None, 'space')
- start_speeds: float32 [4, 3, 2048], P('tm', None, 'space')
The draws below stay inside these ranges and needn't reach their ends.
All inputs are finite; a program needn't handle non-finite values.
Results may differ from the reference program's by a relative error of at most 0.0003.
Values sent between devices are 32-bit elements; how exact they have to be, the bound alone decides.
A program may use at most 64 MiB of HBM per device.

```python
import math
import jax
import jax.numpy as jnp
from jax import lax

NODES = 3
BODIES = 2048
SLICES = 4


def shard_levels(rng, extent, split, low, largest):
    level = 1.0
    for position, blocks in split:
        heights = jax.random.uniform(jax.random.fold_in(jax.random.fold_in(rng, 6), position), (blocks,), jnp.float32, low / len(split), largest / len(split))
        level = level * jnp.repeat(jnp.exp(heights), extent[position] // blocks).reshape((-1,) + (1,) * (len(extent) - 1 - position))
    return level


def gaussian(own_key, extent, width, limit, split=(), held_as=jnp.bfloat16):
    entries = jax.random.normal(own_key, extent, jnp.float32) * width
    if len(split) > 0:
        entries = shard_levels(own_key, extent, split, -0.22, 0.18) * entries
    return jnp.clip(entries, min=-limit, max=limit).astype(held_as)


def setup_inputs(seed: int = 0) -> dict:
    key_of = jax.random.split(jax.random.key(seed), 6)
    positions = gaussian(key_of[0], (SLICES, NODES, 3, BODIES), 1.0, 4.0, ((0, 4), (3, 8)), jnp.float32)
    velocities = gaussian(key_of[1], (SLICES, NODES, 3, BODIES), 0.5, 3.0, ((0, 4), (3, 8)), jnp.float32)
    masses = jnp.clip(jnp.exp(math.log(2.0) - 2.3025851 * jax.random.uniform(key_of[2], (BODIES,), jnp.float32) ** shard_levels(key_of[2], (BODIES,), ((0, 8),), -0.2, 0.2)), 0.2, 2.0)
    initial_places = gaussian(key_of[3], (3, BODIES), 1.0, 4.0, ((1, 8),), jnp.float32)
    initial_speeds = gaussian(key_of[4], (3, BODIES), 0.5, 3.0, ((1, 8),), jnp.float32)
    return dict(positions=positions, velocities=velocities, masses=masses, initial_places=initial_places, initial_speeds=initial_speeds)


soften = 0.01
slice_length = 0.25
lobatto_weights = ((5.0 / 24.0, 1.0 / 3.0, -1.0 / 24.0), (-1.0 / 24.0, 1.0 / 3.0, 5.0 / 24.0))

def gravity(places, masses):
    body_count = places.shape[1]
    block = math.gcd(body_count, 512)
    row_blocks = jnp.transpose(places.reshape(3, body_count // block, block), (1, 0, 2))
    weighted = places * masses[None, :]

    def one_block(local_places):
        squared = (places[0][None, :] - local_places[0][:, None]) ** 2
        squared = squared + (places[1][None, :] - local_places[1][:, None]) ** 2
        squared = squared + (places[2][None, :] - local_places[2][:, None]) ** 2
        inverse = lax.rsqrt(squared + soften)
        kernel = inverse * inverse * inverse
        attract = jnp.dot(weighted, kernel.T, precision=lax.Precision.HIGHEST)
        kernel_sum = jnp.dot(masses, kernel.T, precision=lax.Precision.HIGHEST)
        return (attract - local_places * kernel_sum[None, :]) / body_count
    results = lax.map(one_block, row_blocks)
    return jnp.transpose(results, (1, 0, 2)).reshape(3, body_count)

def slice_sweep(places, speeds, masses):
    earlier = [gravity(places[node], masses) for node in range(3)]
    new_places = [places[0]]
    new_speeds = [speeds[0]]
    new_force = [earlier[0]]
    half_step = 0.5 * slice_length
    for node in range(2):
        weights = lobatto_weights[node]
        moved = slice_length * (weights[0] * speeds[0] + weights[1] * speeds[1] + weights[2] * speeds[2])
        kicked = slice_length * (weights[0] * earlier[0] + weights[1] * earlier[1] + weights[2] * earlier[2])
        place = new_places[node] + half_step * (new_speeds[node] - speeds[node]) + moved
        speed = new_speeds[node] + half_step * (new_force[node] - earlier[node]) + kicked
        new_places.append(place)
        new_speeds.append(speed)
        new_force.append(gravity(place, masses))
    drift_place = new_places[2] - (places[0] + slice_length * speeds[0])
    drift_speed = new_speeds[2] - speeds[0]
    return (jnp.stack(new_places[1:]), jnp.stack(new_speeds[1:]), new_force[2], drift_place, drift_speed)

def reference(positions, velocities, masses, initial_places, initial_speeds):

    def per_slice(couple):
        return slice_sweep(couple[0], couple[1], masses)
    node_places, node_speeds, end_force, drift_place, drift_speed = lax.map(per_slice, (positions, velocities))
    carry_place = initial_places
    carry_speed = initial_speeds
    start_list = []
    speed_list = []
    for slice_number in range(SLICES):
        start_list.append(carry_place)
        speed_list.append(carry_speed)
        carry_place = carry_place + slice_length * carry_speed + drift_place[slice_number]
        carry_speed = carry_speed + drift_speed[slice_number]
    return (node_places, node_speeds, end_force, jnp.stack(start_list), jnp.stack(speed_list))
```

```python
import functools
import jax
import jax.numpy as jnp
from jax import lax
from jax.experimental import pallas as pl
from jax.experimental.pallas import tpu as pltpu
from jax.sharding import PartitionSpec as P

soften = 0.01
slice_length = 0.25
lobatto_weights = ((5.0 / 24.0, 1.0 / 3.0, -1.0 / 24.0), (-1.0 / 24.0, 1.0 / 3.0, 5.0 / 24.0))
LANES = 128
MESH = pl.DeviceIdType.MESH


def round_up(value, step):
    return (value + step - 1) // step * step


def target_of(me, step, count):
    if count & (count - 1) == 0:
        peer, bit = 0, 1
        while bit < count:
            peer = peer + ((me // bit + step // bit) % 2) * bit
            bit *= 2
        return peer
    return (me + step) % count


def source_of(me, step, count):
    if count & (count - 1) == 0:
        return target_of(me, step, count)
    return (me + count - step) % count


def kernel(
    n, slices, body_count, chunk,
    pos, vel, mass, place0, speed0,
    places_out, speeds_out, force_out, start_out, start_speed_out,
    old, first, last, drift, speeds, own, load_sem, wide, total,
    send_old, recv_old, send_first, recv_first, send_last, recv_last, send_drift, recv_drift, ready, go,
):
    me = lax.axis_index("space")
    slot = lax.axis_index("tm")
    halves = mass.shape[0]
    block = halves * LANES
    rows = 3 * halves
    weigh = rows
    base = (0, rows + halves, 2 * rows + halves)
    used = 3 * rows + halves
    f32 = jnp.float32

    barrier = pltpu.get_barrier_semaphore()
    for step in range(1, n):
        pl.semaphore_signal(barrier, inc=1, device_id={"space": target_of(me, step, n)}, device_id_type=MESH)

    @pl.when(me == 0)
    def _():
        for step in range(1, slices):
            pl.semaphore_signal(barrier, inc=1, device_id={"tm": (slot + step) % slices}, device_id_type=MESH)

    loads = [
        pltpu.make_async_copy(mass.at[:, 0, :], old.at[me, pl.ds(weigh, halves), :], load_sem.at[0]),
        pltpu.make_async_copy(place0, own.at[0], load_sem.at[1]),
        pltpu.make_async_copy(speed0, own.at[1], load_sem.at[2]),
    ]
    for node in range(3):
        span = pl.ds(node * rows, rows)
        loads.append(pltpu.make_async_copy(pos.at[span, 0, :], old.at[me, pl.ds(base[node], rows), :], load_sem.at[3 + node]))
        loads.append(pltpu.make_async_copy(vel.at[span, 0, :], speeds.at[node, pl.ds(0, rows), :], load_sem.at[6 + node]))
    for load in loads:
        load.start()
    for load in loads:
        load.wait()

    def copy(ref, count, send, recv, step):
        span = pl.ds(0, count)
        return pltpu.make_async_remote_copy(
            src_ref=ref.at[me, span, :], dst_ref=ref.at[me, span, :], send_sem=send.at[step], recv_sem=recv.at[step],
            device_id={"space": target_of(me, step, n)}, device_id_type=MESH,
        )

    def arrival(ref, count, send, recv, step):
        whose = source_of(me, step, n)
        span = pl.ds(0, count)
        pltpu.make_async_remote_copy(
            src_ref=ref.at[whose, span, :], dst_ref=ref.at[whose, span, :], send_sem=send.at[step], recv_sem=recv.at[step],
            device_id={"space": target_of(me, step, n)}, device_id_type=MESH,
        ).wait_recv()
        return whose

    pl.semaphore_wait(barrier, n - 1 + jnp.where(me == 0, slices - 1, 0))
    for step in range(1, n):
        copy(old, used, send_old, recv_old, step).start()

    speed = [speeds[node, pl.ds(0, rows), :] for node in range(3)]
    x0 = old[me, pl.ds(0, rows), :]
    half_step = 0.5 * slice_length

    def moved(weights):
        return slice_length * (weights[0] * speed[0] + weights[1] * speed[1] + weights[2] * speed[2])

    x1 = x0 + half_step * (speed[0] - speed[0]) + moved(lobatto_weights[0])
    first[me, pl.ds(0, rows), :] = x1
    for step in range(1, n):
        copy(first, rows, send_first, recv_first, step).start()

    @pl.when(me == 0)
    def _():
        for step in range(1, slices):
            pl.semaphore_signal(ready, inc=1, device_id={"tm": (slot + step) % slices}, device_id_type=MESH)

    def lanes_of(half):
        return pl.ds(half * LANES, LANES)

    def widen(node, ref, offset):
        for comp in range(3):
            for half in range(halves):
                line = ref[me, pl.ds(offset + comp * halves + half, 1), :]
                wide[node, comp, lanes_of(half), :] = jnp.broadcast_to(line, (LANES, LANES)).T

    def pairs(whose, parts, fresh):
        def one_chunk(index, carry):
            span = pl.ds(pl.multiple_of(index * chunk, chunk), chunk)
            for node, ref, offset in parts:
                here = [wide[node, comp, span, :] for comp in range(3)]
                sums = [None] * 3 if fresh else [total[node, comp, span, :] for comp in range(3)]
                for half in range(halves):
                    gap = [ref[whose, pl.ds(offset + comp * halves + half, 1), :] - here[comp] for comp in range(3)]
                    weight = old[whose, pl.ds(weigh + half, 1), :]
                    squared = gap[0] * gap[0] + gap[1] * gap[1] + gap[2] * gap[2]
                    inverse = lax.rsqrt(squared + soften)
                    pull = (inverse * inverse) * (inverse * weight)
                    sums = [pull * gap[comp] if sums[comp] is None else sums[comp] + pull * gap[comp] for comp in range(3)]
                for comp in range(3):
                    total[node, comp, span, :] = sums[comp]
            return carry

        lax.fori_loop(0, block // chunk, one_chunk, 0)

    ones = jnp.ones((8, 2 * LANES), jnp.bfloat16)

    def folded(comps):
        parts = []
        for comp in range(3):
            sums = comps[comp]
            high = sums.astype(jnp.bfloat16)
            low = (sums - high.astype(f32)).astype(jnp.bfloat16)
            both = jnp.concatenate([high, low], axis=1)
            line = lax.dot_general(ones, both, (((1,), (1,)), ((), ())), preferred_element_type=f32)
            parts.extend(line[0:1, half * LANES:(half + 1) * LANES] for half in range(halves))
        return jnp.concatenate(parts, axis=0) / body_count

    def added(node):
        return [total[node, comp] for comp in range(3)]

    old_parts = [(node, old, base[node]) for node in range(3)]

    def use_old(whose, fresh):
        pairs(whose, old_parts, fresh)

    def use_new(node, ref, whose, fresh):
        if fresh:
            widen(node, ref, 0)
        pairs(whose, [(node, ref, 0)], fresh)

    for node in range(3):
        widen(node, old, base[node])
    use_old(me, True)

    def with_old(step, carry):
        use_old(arrival(old, used, send_old, recv_old, step), False)
        return carry

    lax.fori_loop(1, n, with_old, 0)

    def kicked(weights, drop):
        parts = [weights[node] * slice_length for node in range(3)]
        parts[1] = parts[1] - drop
        return folded([parts[0] * total[0, comp] + parts[1] * total[1, comp] + parts[2] * total[2, comp] for comp in range(3)])

    v0 = speed[0]
    v1 = v0 + kicked(lobatto_weights[0], 0.0)
    x2 = x1 + half_step * (v1 - speed[1]) + moved(lobatto_weights[1])
    last[me, pl.ds(0, rows), :] = x2
    for step in range(1, n):
        copy(last, rows, send_last, recv_last, step).start()

    @pl.when(me == 0)
    def _():
        pl.semaphore_wait(ready, slices - 1)
        for step in range(1, n):
            pl.semaphore_signal(go, inc=1, device_id={"space": step}, device_id_type=MESH)

    kick = kicked(lobatto_weights[1], half_step)
    use_new(3, first, me, True)

    def only_first(step, carry):
        use_new(3, first, arrival(first, rows, send_first, recv_first, step), False)
        return carry

    lax.fori_loop(1, n, only_first, 0)
    a1 = folded(added(3))
    v2 = v1 + half_step * a1 + kick
    drift_rows = drift.shape[1] // 2
    drift[slot, pl.ds(0, rows), :] = x2 - (x0 + slice_length * v0)
    drift[slot, pl.ds(drift_rows, rows), :] = v2 - v0

    def drift_copy(step, whose, to):
        return pltpu.make_async_remote_copy(
            src_ref=drift.at[whose], dst_ref=drift.at[whose], send_sem=send_drift.at[step], recv_sem=recv_drift.at[step],
            device_id={"tm": to}, device_id_type=MESH,
        )

    @pl.when(me != 0)
    def _():
        pl.semaphore_wait(go, 1)

    for step in range(1, slices):
        @pl.when(slot + step < slices)
        def _():
            drift_copy(step, slot, slot + step).start()

    use_new(4, last, me, True)

    def put(ref, value):
        for row in range(rows):
            ref[row] = value[row:row + 1, :]

    def put_pair(ref, value1, value2):
        for comp in range(3):
            for half in range(halves):
                row = comp * halves + half
                ref[comp, half, 0:1, :] = value1[row:row + 1, :]
                ref[comp, half, 1:2, :] = value2[row:row + 1, :]

    put_pair(places_out, x1, x2)
    put_pair(speeds_out, v1, v2)

    def in_rows(value):
        return jnp.concatenate(
            [value[comp:comp + 1, half * LANES:(half + 1) * LANES] for comp in range(3) for half in range(halves)], axis=0
        )

    start_speed = in_rows(own[1])
    put(start_speed_out, start_speed)
    put(start_out, in_rows(own[0]) + slot.astype(f32) * slice_length * start_speed)

    def only_last(step, carry):
        use_new(4, last, arrival(last, rows, send_last, recv_last, step), False)
        return carry

    lax.fori_loop(1, n, only_last, 0)
    put(force_out, folded(added(4)))

    for step in range(1, slices):
        @pl.when(slot >= step)
        def _():
            whose = slot - step
            drift_copy(step, whose, whose).wait_recv()
            moved_place = drift[whose, pl.ds(0, rows), :]
            moved_speed = drift[whose, pl.ds(drift_rows, rows), :]
            ahead = moved_place + ((step - 1) * slice_length) * moved_speed
            for row in range(rows):
                start_out[row] = start_out[row] + ahead[row:row + 1, :]
                start_speed_out[row] = start_speed_out[row] + moved_speed[row:row + 1, :]

    for step in range(1, n):
        copy(old, used, send_old, recv_old, step).wait_send()
        copy(first, rows, send_first, recv_first, step).wait_send()
        copy(last, rows, send_last, recv_last, step).wait_send()
    for step in range(1, slices):
        @pl.when(slot + step < slices)
        def _():
            drift_copy(step, slot, slot + step).wait_send()


def write_out(*refs):
    copies = [pltpu.make_async_copy(refs[i], refs[5 + i], refs[10].at[i]) for i in range(5)]
    for copy in copies:
        copy.start()
    for copy in copies:
        copy.wait()


def solution(mesh):
    n, slices = mesh.shape["space"], mesh.shape["tm"]

    def body(positions, velocities, masses, initial_places, initial_speeds):
        block = positions.shape[3]
        halves = block // LANES
        stack = round_up(10 * halves, 8)
        part = round_up(3 * halves, 8)
        f32 = jnp.float32
        vmem = pl.BlockSpec(memory_space=pltpu.VMEM)
        dma = pltpu.SemaphoreType.DMA
        rows = 3 * halves
        shapes = [(3, halves, 2, LANES)] * 2 + [(rows, 1, LANES)] * 3
        anywhere = pl.BlockSpec(memory_space=pl.ANY)
        outs = pl.pallas_call(
            functools.partial(kernel, n, slices, float(block * n), 64),
            out_shape=tuple(pltpu.VMEM(shape, f32) for shape in shapes),
            in_specs=[anywhere] * 5,
            out_specs=(vmem,) * 5,
            scratch_shapes=[
                pltpu.VMEM((n, stack, LANES), f32),
                pltpu.VMEM((n, part, LANES), f32),
                pltpu.VMEM((n, part, LANES), f32),
                pltpu.VMEM((slices, 2 * part, LANES), f32),
                pltpu.VMEM((3, part, LANES), f32),
                pltpu.VMEM((2, 3, block), f32),
                dma((9,)),
                pltpu.VMEM((5, 3, block, LANES), f32),
                pltpu.VMEM((5, 3, block, LANES), f32),
                dma((n,)), dma((n,)), dma((n,)), dma((n,)), dma((n,)), dma((n,)),
                dma((slices,)), dma((slices,)),
                pltpu.SemaphoreType.REGULAR, pltpu.SemaphoreType.REGULAR,
            ],
            compiler_params=pltpu.CompilerParams(collective_id=0, has_side_effects=True),
        )(
            positions.reshape(3 * rows, 1, LANES),
            velocities.reshape(3 * rows, 1, LANES),
            masses.reshape(halves, 1, LANES),
            initial_places,
            initial_speeds,
        )
        outs = pl.pallas_call(
            write_out,
            out_shape=tuple(jax.ShapeDtypeStruct(shape, f32) for shape in shapes),
            in_specs=[vmem] * 5,
            out_specs=(anywhere,) * 5,
            scratch_shapes=[dma((5,))],
        )(*(pltpu.with_memory_space_constraint(part, pltpu.VMEM) for part in outs))
        paired = [part.transpose(2, 0, 1, 3).reshape(1, 2, 3, block) for part in outs[:2]]
        return (*paired, *(part.reshape(1, 3, block) for part in outs[2:]))

    return jax.shard_map(
        body,
        mesh=mesh,
        in_specs=(
            P("tm", None, None, "space"),
            P("tm", None, None, "space"),
            P("space"),
            P(None, "space"),
            P(None, "space"),
        ),
        out_specs=(
            P("tm", None, None, "space"),
            P("tm", None, None, "space"),
            P("tm", None, "space"),
            P("tm", None, "space"),
            P("tm", None, "space"),
        ),
        check_vma=False,
    )
```

```python
import functools
import jax
import jax.numpy as jnp
from jax import lax
from jax.experimental import pallas as pl
from jax.experimental.pallas import tpu as pltpu
from jax.sharding import PartitionSpec as P

soften = 0.01
slice_length = 0.25
lobatto_weights = ((5.0 / 24.0, 1.0 / 3.0, -1.0 / 24.0), (-1.0 / 24.0, 1.0 / 3.0, 5.0 / 24.0))
LANES = 128
MESH = pl.DeviceIdType.MESH


def round_up(value, step):
    return (value + step - 1) // step * step


def target_of(me, step, count):
    if count & (count - 1) == 0:
        peer, bit = 0, 1
        while bit < count:
            peer = peer + ((me // bit + step // bit) % 2) * bit
            bit *= 2
        return peer
    return (me + step) % count


def source_of(me, step, count):
    if count & (count - 1) == 0:
        return target_of(me, step, count)
    return (me + count - step) % count


def kernel(
    n, slices, body_count, chunk,
    pos, vel, mass, place0, speed0,
    places_out, speeds_out, force_out, start_out, start_speed_out,
    old, first, last, drift, speeds, own, load_sem, wide, total,
    send_old, recv_old, send_first, recv_first, send_last, recv_last, send_drift, recv_drift, ready, go, arrive,
):
    me = lax.axis_index("space")
    slot = lax.axis_index("tm")
    halves = mass.shape[0]
    block = halves * LANES
    rows = 3 * halves
    weigh = rows
    base = (0, rows + halves, 2 * rows + halves)
    used = 3 * rows + halves
    f32 = jnp.float32

    leader = 0
    barrier = pltpu.get_barrier_semaphore()
    for other in range(1, n):
        @pl.when(other > me)
        def _():
            pl.semaphore_signal(barrier, inc=1, device_id={"space": other}, device_id_type=MESH)

    @pl.when(me == leader)
    def _():
        for step in range(1, slices):
            pl.semaphore_signal(barrier, inc=1, device_id={"tm": (slot + step) % slices}, device_id_type=MESH)

    loads = [
        pltpu.make_async_copy(mass.at[:, 0, :], old.at[me, pl.ds(weigh, halves), :], load_sem.at[0]),
        pltpu.make_async_copy(place0, own.at[0], load_sem.at[1]),
        pltpu.make_async_copy(speed0, own.at[1], load_sem.at[2]),
    ]
    for node in range(3):
        span = pl.ds(node * rows, rows)
        loads.append(pltpu.make_async_copy(pos.at[span, 0, :], old.at[me, pl.ds(base[node], rows), :], load_sem.at[3 + node]))
        loads.append(pltpu.make_async_copy(vel.at[span, 0, :], speeds.at[node, pl.ds(0, rows), :], load_sem.at[6 + node]))
    for load in loads:
        load.start()

    @pl.when(me > 0)
    def _():
        pl.semaphore_wait(barrier, me)

    for other in range(n - 1):
        @pl.when(other < me)
        def _():
            pl.semaphore_signal(arrive.at[me], inc=1, device_id={"space": other}, device_id_type=MESH)

    for load in loads:
        load.wait()

    chips = n // 2
    chip, core = me // 2, me % 2

    def copy(ref, count, send, recv, to):
        span = pl.ds(0, count)
        return pltpu.make_async_remote_copy(
            src_ref=ref.at[me, span, :], dst_ref=ref.at[me, span, :], send_sem=send.at[to], recv_sem=recv.at[me],
            device_id={"space": to}, device_id_type=MESH,
        )

    def whose_at(step):
        far = (step - 2) // 2
        above = chip + 1 + far
        side = (step - 2) % 2
        flip = core + side - 2 * core * side
        other = 2 * jnp.where(above < chips, above, chips - 2 - far) + flip
        return jnp.where(step == 1, me + 1 - 2 * core, other)

    def arrival(ref, count, send, recv, step):
        whose = whose_at(step)
        span = pl.ds(0, count)
        pltpu.make_async_remote_copy(
            src_ref=ref.at[whose, span, :], dst_ref=ref.at[whose, span, :], send_sem=send.at[whose], recv_sem=recv.at[whose],
            device_id={"space": whose}, device_id_type=MESH,
        ).wait_recv()
        return whose

    def up(index):
        return index + jnp.where(index < me, 0, 1)

    def seq(index):
        if index == 0:
            return me + 1 - 2 * core
        far, side = (index - 1) // 2, (index - 1) % 2
        above = chip + 1 + far
        flip = core + side - 2 * core * side
        return 2 * jnp.where(above < chips, above, chips - 2 - far) + flip

    for other in range(n - 1):
        @pl.when(other < me)
        def _():
            copy(old, used, send_old, recv_old, other).start()

    speed = [speeds[node, pl.ds(0, rows), :] for node in range(3)]
    x0 = old[me, pl.ds(0, rows), :]
    half_step = 0.5 * slice_length

    def moved(weights):
        return slice_length * (weights[0] * speed[0] + weights[1] * speed[1] + weights[2] * speed[2])

    x1 = x0 + half_step * (speed[0] - speed[0]) + moved(lobatto_weights[0])
    first[me, pl.ds(0, rows), :] = x1

    def meet(other):
        pl.semaphore_wait(arrive.at[other], 1)
        copy(old, used, send_old, recv_old, other).start()

    def lanes_of(half):
        return pl.ds(half * LANES, LANES)

    def widen(node, ref, offset):
        for comp in range(3):
            for half in range(halves):
                line = ref[me, pl.ds(offset + comp * halves + half, 1), :]
                wide[node, comp, lanes_of(half), :] = jnp.broadcast_to(line, (LANES, LANES)).T

    def pairs(whose, parts, fresh):
        def one_chunk(index, carry):
            span = pl.ds(pl.multiple_of(index * chunk, chunk), chunk)
            for node, ref, offset in parts:
                here = [wide[node, comp, span, :] for comp in range(3)]
                sums = [None] * 3 if fresh else [total[node, comp, span, :] for comp in range(3)]
                for half in range(halves):
                    gap = [ref[whose, pl.ds(offset + comp * halves + half, 1), :] - here[comp] for comp in range(3)]
                    weight = old[whose, pl.ds(weigh + half, 1), :]
                    squared = gap[0] * gap[0] + gap[1] * gap[1] + gap[2] * gap[2]
                    inverse = lax.rsqrt(squared + soften)
                    pull = (inverse * inverse) * (inverse * weight)
                    sums = [pull * gap[comp] if sums[comp] is None else sums[comp] + pull * gap[comp] for comp in range(3)]
                for comp in range(3):
                    total[node, comp, span, :] = sums[comp]
            return carry

        lax.fori_loop(0, block // chunk, one_chunk, 0)

    ones = jnp.ones((8, 2 * LANES), jnp.bfloat16)

    def folded(comps):
        parts = []
        for comp in range(3):
            sums = comps[comp]
            high = sums.astype(jnp.bfloat16)
            low = (sums - high.astype(f32)).astype(jnp.bfloat16)
            both = jnp.concatenate([high, low], axis=1)
            line = lax.dot_general(ones, both, (((1,), (1,)), ((), ())), preferred_element_type=f32)
            parts.extend(line[0:1, half * LANES:(half + 1) * LANES] for half in range(halves))
        return jnp.concatenate(parts, axis=0) / body_count

    def added(node):
        return [total[node, comp] for comp in range(3)]

    old_parts = [(node, old, base[node]) for node in range(3)]

    def use_old(whose, fresh):
        pairs(whose, old_parts, fresh)

    def use_new(node, ref, whose, fresh):
        if fresh:
            widen(node, ref, 0)
        pairs(whose, [(node, ref, 0)], fresh)

    for node in range(3):
        widen(node, old, base[node])
    near = 2 * chip + 4
    for other in range(1, n):
        @pl.when((other > me) & (other < near))
        def _():
            meet(other)

    use_old(me, True)
    for other in range(1, n):
        @pl.when((other > me) & (other >= near))
        def _():
            meet(other)

    for index in range(n - 1):
        copy(first, rows, send_first, recv_first, seq(index)).start()

    @pl.when(me == leader)
    def _():
        pl.semaphore_wait(barrier, slices - 1)
        for step in range(1, slices):
            pl.semaphore_signal(ready, inc=1, device_id={"tm": (slot + step) % slices}, device_id_type=MESH)


    def with_old(step, carry):
        use_old(arrival(old, used, send_old, recv_old, step), False)
        return carry

    lax.fori_loop(1, n, with_old, 0)

    def kicked(weights, drop):
        parts = [weights[node] * slice_length for node in range(3)]
        parts[1] = parts[1] - drop
        return folded([parts[0] * total[0, comp] + parts[1] * total[1, comp] + parts[2] * total[2, comp] for comp in range(3)])

    v0 = speed[0]
    v1 = v0 + kicked(lobatto_weights[0], 0.0)
    x2 = x1 + half_step * (v1 - speed[1]) + moved(lobatto_weights[1])
    last[me, pl.ds(0, rows), :] = x2
    for index in range(n - 1):
        copy(last, rows, send_last, recv_last, up(index)).start()

    @pl.when(me == leader)
    def _():
        pl.semaphore_wait(ready, slices - 1)
        for other in range(n):
            if other != leader:
                pl.semaphore_signal(go, inc=1, device_id={"space": other}, device_id_type=MESH)

    kick = kicked(lobatto_weights[1], half_step)
    use_new(3, first, me, True)

    def only_first(step, carry):
        use_new(3, first, arrival(first, rows, send_first, recv_first, step), False)
        return carry

    lax.fori_loop(1, n, only_first, 0)
    a1 = folded(added(3))
    v2 = v1 + half_step * a1 + kick
    drift_rows = drift.shape[1] // 2
    drift[slot, pl.ds(0, rows), :] = x2 - (x0 + slice_length * v0)
    drift[slot, pl.ds(drift_rows, rows), :] = v2 - v0

    def drift_copy(step, whose, to):
        return pltpu.make_async_remote_copy(
            src_ref=drift.at[whose], dst_ref=drift.at[whose], send_sem=send_drift.at[step], recv_sem=recv_drift.at[step],
            device_id={"tm": to}, device_id_type=MESH,
        )

    @pl.when(me != leader)
    def _():
        pl.semaphore_wait(go, 1)

    for step in range(1, slices):
        @pl.when(slot + step < slices)
        def _():
            drift_copy(step, slot, slot + step).start()

    use_new(4, last, me, True)

    def put(ref, value):
        for row in range(rows):
            ref[row] = value[row:row + 1, :]

    def put_pair(ref, value1, value2):
        for comp in range(3):
            for half in range(halves):
                row = comp * halves + half
                ref[comp, half, 0:1, :] = value1[row:row + 1, :]
                ref[comp, half, 1:2, :] = value2[row:row + 1, :]

    put_pair(places_out, x1, x2)
    put_pair(speeds_out, v1, v2)

    def in_rows(value):
        return jnp.concatenate(
            [value[comp:comp + 1, half * LANES:(half + 1) * LANES] for comp in range(3) for half in range(halves)], axis=0
        )

    start_speed = in_rows(own[1])
    put(start_speed_out, start_speed)
    put(start_out, in_rows(own[0]) + slot.astype(f32) * slice_length * start_speed)

    def only_last(step, carry):
        use_new(4, last, arrival(last, rows, send_last, recv_last, step), False)
        return carry

    lax.fori_loop(1, n, only_last, 0)
    put(force_out, folded(added(4)))

    for step in range(1, slices):
        @pl.when(slot >= step)
        def _():
            whose = slot - step
            drift_copy(step, whose, whose).wait_recv()
            moved_place = drift[whose, pl.ds(0, rows), :]
            moved_speed = drift[whose, pl.ds(drift_rows, rows), :]
            ahead = moved_place + ((step - 1) * slice_length) * moved_speed
            for row in range(rows):
                start_out[row] = start_out[row] + ahead[row:row + 1, :]
                start_speed_out[row] = start_speed_out[row] + moved_speed[row:row + 1, :]

    for step in range(1, n):
        copy(old, used, send_old, recv_old, target_of(me, step, n)).wait_send()
        copy(first, rows, send_first, recv_first, target_of(me, step, n)).wait_send()
        copy(last, rows, send_last, recv_last, target_of(me, step, n)).wait_send()
    for step in range(1, slices):
        @pl.when(slot + step < slices)
        def _():
            drift_copy(step, slot, slot + step).wait_send()


def write_out(*refs):
    copies = [pltpu.make_async_copy(refs[i], refs[5 + i], refs[10].at[i]) for i in range(5)]
    for copy in copies:
        copy.start()
    for copy in copies:
        copy.wait()


def solution(mesh):
    n, slices = mesh.shape["space"], mesh.shape["tm"]

    def body(positions, velocities, masses, initial_places, initial_speeds):
        block = positions.shape[3]
        halves = block // LANES
        stack = round_up(10 * halves, 8)
        part = round_up(3 * halves, 8)
        f32 = jnp.float32
        vmem = pl.BlockSpec(memory_space=pltpu.VMEM)
        dma = pltpu.SemaphoreType.DMA
        rows = 3 * halves
        shapes = [(3, halves, 2, LANES)] * 2 + [(rows, 1, LANES)] * 3
        anywhere = pl.BlockSpec(memory_space=pl.ANY)
        outs = pl.pallas_call(
            functools.partial(kernel, n, slices, float(block * n), 128),
            out_shape=tuple(pltpu.VMEM(shape, f32) for shape in shapes),
            in_specs=[anywhere] * 5,
            out_specs=(vmem,) * 5,
            scratch_shapes=[
                pltpu.VMEM((n, stack, LANES), f32),
                pltpu.VMEM((n, part, LANES), f32),
                pltpu.VMEM((n, part, LANES), f32),
                pltpu.VMEM((slices, 2 * part, LANES), f32),
                pltpu.VMEM((3, part, LANES), f32),
                pltpu.VMEM((2, 3, block), f32),
                dma((9,)),
                pltpu.VMEM((5, 3, block, LANES), f32),
                pltpu.VMEM((5, 3, block, LANES), f32),
                dma((n,)), dma((n,)), dma((n,)), dma((n,)), dma((n,)), dma((n,)),
                dma((slices,)), dma((slices,)),
                pltpu.SemaphoreType.REGULAR, pltpu.SemaphoreType.REGULAR, pltpu.SemaphoreType.REGULAR((n,)),
            ],
            compiler_params=pltpu.CompilerParams(collective_id=0, has_side_effects=True),
        )(
            positions.reshape(3 * rows, 1, LANES),
            velocities.reshape(3 * rows, 1, LANES),
            masses.reshape(halves, 1, LANES),
            initial_places,
            initial_speeds,
        )
        outs = pl.pallas_call(
            write_out,
            out_shape=tuple(jax.ShapeDtypeStruct(shape, f32) for shape in shapes),
            in_specs=[vmem] * 5,
            out_specs=(anywhere,) * 5,
            scratch_shapes=[dma((5,))],
        )(*(pltpu.with_memory_space_constraint(part, pltpu.VMEM) for part in outs))
        paired = [part.transpose(2, 0, 1, 3).reshape(1, 2, 3, block) for part in outs[:2]]
        return (*paired, *(part.reshape(1, 3, block) for part in outs[2:]))

    return jax.shard_map(
        body,
        mesh=mesh,
        in_specs=(
            P("tm", None, None, "space"),
            P("tm", None, None, "space"),
            P("space"),
            P(None, "space"),
            P(None, "space"),
        ),
        out_specs=(
            P("tm", None, None, "space"),
            P("tm", None, None, "space"),
            P("tm", None, "space"),
            P("tm", None, "space"),
            P("tm", None, "space"),
        ),
        check_vma=False,
    )
```

```python
import functools
import jax
import jax.numpy as jnp
from jax import lax
from jax.experimental import pallas as pl
from jax.experimental.pallas import tpu as pltpu
from jax.sharding import PartitionSpec as P

soften = 0.01
slice_length = 0.25
lobatto_weights = ((5.0 / 24.0, 1.0 / 3.0, -1.0 / 24.0), (-1.0 / 24.0, 1.0 / 3.0, 5.0 / 24.0))
LANES = 128
MESH = pl.DeviceIdType.MESH


def round_up(value, step):
    return (value + step - 1) // step * step


def target_of(me, step, count):
    if count & (count - 1) == 0:
        peer, bit = 0, 1
        while bit < count:
            peer = peer + ((me // bit + step // bit) % 2) * bit
            bit *= 2
        return peer
    return (me + step) % count


def source_of(me, step, count):
    if count & (count - 1) == 0:
        return target_of(me, step, count)
    return (me + count - step) % count


def kernel(
    n, slices, body_count, chunk,
    pos, vel, mass, place0, speed0,
    places_out, speeds_out, force_out, start_out, start_speed_out,
    old, first, last, drift, speeds, own, load_sem, wide, total,
    send_old, recv_old, send_first, recv_first, send_last, recv_last, send_drift, recv_drift, ready, go, arrive,
):
    me = lax.axis_index("space")
    slot = lax.axis_index("tm")
    halves = mass.shape[0]
    block = halves * LANES
    rows = 3 * halves
    weigh = rows
    base = (0, rows + halves, 2 * rows + halves)
    used = 3 * rows + halves
    f32 = jnp.float32

    loads = [
        pltpu.make_async_copy(mass.at[:, 0, :], old.at[me, pl.ds(weigh, halves), :], load_sem.at[0]),
        pltpu.make_async_copy(place0, own.at[0], load_sem.at[1]),
        pltpu.make_async_copy(speed0, own.at[1], load_sem.at[2]),
    ]
    for node in range(3):
        span = pl.ds(node * rows, rows)
        loads.append(pltpu.make_async_copy(pos.at[span, 0, :], old.at[me, pl.ds(base[node], rows), :], load_sem.at[3 + node]))
        loads.append(pltpu.make_async_copy(vel.at[span, 0, :], speeds.at[node, pl.ds(0, rows), :], load_sem.at[6 + node]))
    for load in loads:
        load.start()

    leader = 0
    barrier = pltpu.get_barrier_semaphore()
    for other in range(1, n):
        @pl.when(other > me)
        def _():
            pl.semaphore_signal(barrier, inc=1, device_id={"space": other}, device_id_type=MESH)

    @pl.when(me == leader)
    def _():
        for step in range(1, slices):
            pl.semaphore_signal(barrier, inc=1, device_id={"tm": (slot + step) % slices}, device_id_type=MESH)

    @pl.when(me > 0)
    def _():
        pl.semaphore_wait(barrier, me)

    for other in range(n - 1):
        @pl.when(other < me)
        def _():
            pl.semaphore_signal(arrive.at[me], inc=1, device_id={"space": other}, device_id_type=MESH)

    for load in loads:
        load.wait()

    chips = n // 2
    chip, core = me // 2, me % 2

    def copy(ref, count, send, recv, to):
        span = pl.ds(0, count)
        return pltpu.make_async_remote_copy(
            src_ref=ref.at[me, span, :], dst_ref=ref.at[me, span, :], send_sem=send.at[to], recv_sem=recv.at[me],
            device_id={"space": to}, device_id_type=MESH,
        )

    def whose_at(step):
        far = (step - 2) // 2
        side = (step - 2) % 2
        flip = core + side - 2 * core * side
        other = 2 * jnp.where(far < chip, chip - 1 - far, far + 1) + flip
        return jnp.where(step == 1, me + 1 - 2 * core, other)

    def arrival(ref, count, send, recv, step):
        whose = whose_at(step)
        span = pl.ds(0, count)
        pltpu.make_async_remote_copy(
            src_ref=ref.at[whose, span, :], dst_ref=ref.at[whose, span, :], send_sem=send.at[whose], recv_sem=recv.at[whose],
            device_id={"space": whose}, device_id_type=MESH,
        ).wait_recv()
        return whose

    def up(index):
        return index + jnp.where(index < me, 0, 1)

    def seq(index):
        if index == 0:
            return me + 1 - 2 * core
        far, side = (index - 1) // 2, (index - 1) % 2
        above = chip + 1 + far
        flip = core + side - 2 * core * side
        return 2 * jnp.where(above < chips, above, chips - 2 - far) + flip

    for other in range(n - 1):
        @pl.when(other < me)
        def _():
            copy(old, used, send_old, recv_old, other).start()

    speed = [speeds[node, pl.ds(0, rows), :] for node in range(3)]
    x0 = old[me, pl.ds(0, rows), :]
    half_step = 0.5 * slice_length

    def moved(weights):
        return slice_length * (weights[0] * speed[0] + weights[1] * speed[1] + weights[2] * speed[2])

    x1 = x0 + half_step * (speed[0] - speed[0]) + moved(lobatto_weights[0])
    first[me, pl.ds(0, rows), :] = x1

    def meet(other):
        pl.semaphore_wait(arrive.at[other], 1)
        copy(old, used, send_old, recv_old, other).start()

    def lanes_of(half):
        return pl.ds(half * LANES, LANES)

    def widen(node, ref, offset):
        for comp in range(3):
            for half in range(halves):
                line = ref[me, pl.ds(offset + comp * halves + half, 1), :]
                wide[node, comp, lanes_of(half), :] = jnp.broadcast_to(line, (LANES, LANES)).T

    def pairs(whose, parts, fresh):
        def one_chunk(index, carry):
            span = pl.ds(pl.multiple_of(index * chunk, chunk), chunk)
            for node, ref, offset in parts:
                here = [wide[node, comp, span, :] for comp in range(3)]
                sums = [None] * 3 if fresh else [total[node, comp, span, :] for comp in range(3)]
                for half in range(halves):
                    gap = [ref[whose, pl.ds(offset + comp * halves + half, 1), :] - here[comp] for comp in range(3)]
                    weight = old[whose, pl.ds(weigh + half, 1), :]
                    squared = gap[0] * gap[0] + gap[1] * gap[1] + gap[2] * gap[2]
                    inverse = lax.rsqrt(squared + soften)
                    pull = (inverse * inverse) * (inverse * weight)
                    sums = [pull * gap[comp] if sums[comp] is None else sums[comp] + pull * gap[comp] for comp in range(3)]
                for comp in range(3):
                    total[node, comp, span, :] = sums[comp]
            return carry

        lax.fori_loop(0, block // chunk, one_chunk, 0)

    ones = jnp.ones((8, 2 * LANES), jnp.bfloat16)

    def folded(comps):
        parts = []
        for comp in range(3):
            for half in range(halves):
                turned = comps[comp][half * LANES:(half + 1) * LANES, :].T
                parts.append(jnp.sum(turned, axis=0, keepdims=True))
        return jnp.concatenate(parts, axis=0) / body_count

    def added(node):
        return [total[node, comp] for comp in range(3)]

    old_parts = [(node, old, base[node]) for node in range(3)]

    def use_old(whose, fresh):
        pairs(whose, old_parts, fresh)

    def use_new(node, ref, whose, fresh):
        if fresh:
            widen(node, ref, 0)
        pairs(whose, [(node, ref, 0)], fresh)

    for node in range(3):
        widen(node, old, base[node])
    near = 2 * chip + 4
    for other in range(1, n):
        @pl.when((other > me) & (other < near))
        def _():
            meet(other)

    use_old(me, True)
    for other in range(1, n):
        @pl.when((other > me) & (other >= near))
        def _():
            meet(other)

    for index in range(n - 1):
        copy(first, rows, send_first, recv_first, seq(index)).start()

    @pl.when(me == leader)
    def _():
        pl.semaphore_wait(barrier, slices - 1)
        for step in range(1, slices):
            pl.semaphore_signal(ready, inc=1, device_id={"tm": (slot + step) % slices}, device_id_type=MESH)


    def with_old(step, carry):
        use_old(arrival(old, used, send_old, recv_old, step), False)
        return carry

    lax.fori_loop(1, n, with_old, 0)

    def kicked(weights, drop):
        parts = [weights[node] * slice_length for node in range(3)]
        parts[1] = parts[1] - drop
        return folded([parts[0] * total[0, comp] + parts[1] * total[1, comp] + parts[2] * total[2, comp] for comp in range(3)])

    v0 = speed[0]
    v1 = v0 + kicked(lobatto_weights[0], 0.0)
    x2 = x1 + half_step * (v1 - speed[1]) + moved(lobatto_weights[1])
    last[me, pl.ds(0, rows), :] = x2
    for index in range(n - 1):
        copy(last, rows, send_last, recv_last, up(index)).start()

    @pl.when(me == leader)
    def _():
        pl.semaphore_wait(ready, slices - 1)
        for other in range(n):
            if other != leader:
                pl.semaphore_signal(go, inc=1, device_id={"space": other}, device_id_type=MESH)

    kick = kicked(lobatto_weights[1], half_step)
    use_new(3, first, me, True)

    def only_first(step, carry):
        use_new(3, first, arrival(first, rows, send_first, recv_first, step), False)
        return carry

    lax.fori_loop(1, n, only_first, 0)
    a1 = folded(added(3))
    v2 = v1 + half_step * a1 + kick
    drift_rows = drift.shape[1] // 2
    drift[slot, pl.ds(0, rows), :] = x2 - (x0 + slice_length * v0)
    drift[slot, pl.ds(drift_rows, rows), :] = v2 - v0

    def drift_copy(step, whose, to):
        return pltpu.make_async_remote_copy(
            src_ref=drift.at[whose], dst_ref=drift.at[whose], send_sem=send_drift.at[step], recv_sem=recv_drift.at[step],
            device_id={"tm": to}, device_id_type=MESH,
        )

    @pl.when(me != leader)
    def _():
        pl.semaphore_wait(go, 1)

    for step in range(1, slices):
        @pl.when(slot + step < slices)
        def _():
            drift_copy(step, slot, slot + step).start()

    use_new(4, last, me, True)

    def put(ref, value):
        for row in range(rows):
            ref[row] = value[row:row + 1, :]

    def put_pair(ref, value1, value2):
        for comp in range(3):
            for half in range(halves):
                row = comp * halves + half
                ref[comp, half, 0:1, :] = value1[row:row + 1, :]
                ref[comp, half, 1:2, :] = value2[row:row + 1, :]

    put_pair(places_out, x1, x2)
    put_pair(speeds_out, v1, v2)

    def in_rows(value):
        return jnp.concatenate(
            [value[comp:comp + 1, half * LANES:(half + 1) * LANES] for comp in range(3) for half in range(halves)], axis=0
        )

    start_speed = in_rows(own[1])
    put(start_speed_out, start_speed)
    put(start_out, in_rows(own[0]) + slot.astype(f32) * slice_length * start_speed)

    for step in range(1, n):
        copy(old, used, send_old, recv_old, target_of(me, step, n)).wait_send()
        copy(first, rows, send_first, recv_first, target_of(me, step, n)).wait_send()

    for step in range(1, n):
        copy(last, rows, send_last, recv_last, target_of(me, step, n)).wait_send()

    def only_last(step, carry):
        use_new(4, last, arrival(last, rows, send_last, recv_last, step), False)
        return carry

    lax.fori_loop(1, n, only_last, 0)
    put(force_out, folded(added(4)))

    for step in range(1, slices):
        @pl.when(slot >= step)
        def _():
            whose = slot - step
            drift_copy(step, whose, whose).wait_recv()
            moved_place = drift[whose, pl.ds(0, rows), :]
            moved_speed = drift[whose, pl.ds(drift_rows, rows), :]
            ahead = moved_place + ((step - 1) * slice_length) * moved_speed
            for row in range(rows):
                start_out[row] = start_out[row] + ahead[row:row + 1, :]
                start_speed_out[row] = start_speed_out[row] + moved_speed[row:row + 1, :]

    for step in range(1, slices):
        @pl.when(slot + step < slices)
        def _():
            drift_copy(step, slot, slot + step).wait_send()


def write_out(*refs):
    copies = [pltpu.make_async_copy(refs[i], refs[5 + i], refs[10].at[i]) for i in range(5)]
    for copy in copies:
        copy.start()
    for copy in copies:
        copy.wait()


def solution(mesh):
    n, slices = mesh.shape["space"], mesh.shape["tm"]

    def body(positions, velocities, masses, initial_places, initial_speeds):
        block = positions.shape[3]
        halves = block // LANES
        stack = round_up(10 * halves, 8)
        part = round_up(3 * halves, 8)
        f32 = jnp.float32
        vmem = pl.BlockSpec(memory_space=pltpu.VMEM)
        dma = pltpu.SemaphoreType.DMA
        rows = 3 * halves
        shapes = [(3, halves, 2, LANES)] * 2 + [(rows, 1, LANES)] * 3
        anywhere = pl.BlockSpec(memory_space=pl.ANY)
        outs = pl.pallas_call(
            functools.partial(kernel, n, slices, float(block * n), 64),
            out_shape=tuple(pltpu.VMEM(shape, f32) for shape in shapes),
            in_specs=[anywhere] * 5,
            out_specs=(vmem,) * 5,
            scratch_shapes=[
                pltpu.VMEM((n, stack, LANES), f32),
                pltpu.VMEM((n, part, LANES), f32),
                pltpu.VMEM((n, part, LANES), f32),
                pltpu.VMEM((slices, 2 * part, LANES), f32),
                pltpu.VMEM((3, part, LANES), f32),
                pltpu.VMEM((2, 3, block), f32),
                dma((9,)),
                pltpu.VMEM((5, 3, block, LANES), f32),
                pltpu.VMEM((5, 3, block, LANES), f32),
                dma((n,)), dma((n,)), dma((n,)), dma((n,)), dma((n,)), dma((n,)),
                dma((slices,)), dma((slices,)),
                pltpu.SemaphoreType.REGULAR, pltpu.SemaphoreType.REGULAR, pltpu.SemaphoreType.REGULAR((n,)),
            ],
            compiler_params=pltpu.CompilerParams(collective_id=0, has_side_effects=True),
        )(
            positions.reshape(3 * rows, 1, LANES),
            velocities.reshape(3 * rows, 1, LANES),
            masses.reshape(halves, 1, LANES),
            initial_places,
            initial_speeds,
        )
        outs = pl.pallas_call(
            write_out,
            out_shape=tuple(jax.ShapeDtypeStruct(shape, f32) for shape in shapes),
            in_specs=[vmem] * 5,
            out_specs=(anywhere,) * 5,
            scratch_shapes=[dma((5,))],
        )(*(pltpu.with_memory_space_constraint(part, pltpu.VMEM) for part in outs))
        paired = [part.transpose(2, 0, 1, 3).reshape(1, 2, 3, block) for part in outs[:2]]
        return (*paired, *(part.reshape(1, 3, block) for part in outs[2:]))

    return jax.shard_map(
        body,
        mesh=mesh,
        in_specs=(
            P("tm", None, None, "space"),
            P("tm", None, None, "space"),
            P("space"),
            P(None, "space"),
            P(None, "space"),
        ),
        out_specs=(
            P("tm", None, None, "space"),
            P("tm", None, None, "space"),
            P("tm", None, "space"),
            P("tm", None, "space"),
            P("tm", None, "space"),
        ),
        check_vma=False,
    )
```

```python
import functools
import jax
import jax.numpy as jnp
from jax import lax
from jax.experimental import pallas as pl
from jax.experimental.pallas import tpu as pltpu
from jax.sharding import PartitionSpec as P

soften = 0.01
slice_length = 0.25
lobatto_weights = ((5.0 / 24.0, 1.0 / 3.0, -1.0 / 24.0), (-1.0 / 24.0, 1.0 / 3.0, 5.0 / 24.0))
LANES = 128
MESH = pl.DeviceIdType.MESH


def round_up(value, step):
    return (value + step - 1) // step * step


def target_of(me, step, count):
    if count & (count - 1) == 0:
        peer, bit = 0, 1
        while bit < count:
            peer = peer + ((me // bit + step // bit) % 2) * bit
            bit *= 2
        return peer
    return (me + step) % count


def source_of(me, step, count):
    if count & (count - 1) == 0:
        return target_of(me, step, count)
    return (me + count - step) % count


def kernel(
    n, slices, body_count, chunk,
    pos, vel, mass, place0, speed0,
    places_out, speeds_out, force_out, start_out, start_speed_out,
    old, first, last, drift, speeds, own, load_sem, wide, total,
    send_old, recv_old, send_first, recv_first, send_last, recv_last, send_drift, recv_drift, ready, go, arrive,
):
    me = lax.axis_index("space")
    slot = lax.axis_index("tm")
    halves = mass.shape[0]
    block = halves * LANES
    rows = 3 * halves
    weigh = rows
    base = (0, rows + halves, 2 * rows + halves)
    used = 3 * rows + halves
    f32 = jnp.float32

    loads = [
        pltpu.make_async_copy(mass.at[:, 0, :], old.at[me, pl.ds(weigh, halves), :], load_sem.at[0]),
        pltpu.make_async_copy(place0, own.at[0], load_sem.at[1]),
        pltpu.make_async_copy(speed0, own.at[1], load_sem.at[2]),
    ]
    for node in range(3):
        span = pl.ds(node * rows, rows)
        loads.append(pltpu.make_async_copy(pos.at[span, 0, :], old.at[me, pl.ds(base[node], rows), :], load_sem.at[3 + node]))
        loads.append(pltpu.make_async_copy(vel.at[span, 0, :], speeds.at[node, pl.ds(0, rows), :], load_sem.at[6 + node]))
    for load in loads:
        load.start()

    leader = 0
    barrier = pltpu.get_barrier_semaphore()
    for other in range(1, n):
        @pl.when(other > me)
        def _():
            pl.semaphore_signal(barrier, inc=1, device_id={"space": other}, device_id_type=MESH)

    @pl.when(me == leader)
    def _():
        for step in range(1, slices):
            pl.semaphore_signal(barrier, inc=1, device_id={"tm": (slot + step) % slices}, device_id_type=MESH)

    @pl.when(me > 0)
    def _():
        pl.semaphore_wait(barrier, me)

    for other in range(n - 1):
        @pl.when(other < me)
        def _():
            pl.semaphore_signal(arrive.at[me], inc=1, device_id={"space": other}, device_id_type=MESH)

    for load in loads:
        load.wait()

    chips = n // 2
    chip, core = me // 2, me % 2

    def copy(ref, count, send, recv, to):
        span = pl.ds(0, count)
        return pltpu.make_async_remote_copy(
            src_ref=ref.at[me, span, :], dst_ref=ref.at[me, span, :], send_sem=send.at[to], recv_sem=recv.at[me],
            device_id={"space": to}, device_id_type=MESH,
        )

    def whose_at(step):
        far = (step - 2) // 2
        side = (step - 2) % 2
        flip = core + side - 2 * core * side
        other = 2 * jnp.where(far < chip, chip - 1 - far, far + 1) + flip
        return jnp.where(step == 1, me + 1 - 2 * core, other)

    def arrival(ref, count, send, recv, step):
        whose = whose_at(step)
        span = pl.ds(0, count)
        pltpu.make_async_remote_copy(
            src_ref=ref.at[whose, span, :], dst_ref=ref.at[whose, span, :], send_sem=send.at[whose], recv_sem=recv.at[whose],
            device_id={"space": whose}, device_id_type=MESH,
        ).wait_recv()
        return whose

    def up(index):
        return index + jnp.where(index < me, 0, 1)

    def seq(index):
        if index == 0:
            return me + 1 - 2 * core
        far, side = (index - 1) // 2, (index - 1) % 2
        above = chip + 1 + far
        flip = core + side - 2 * core * side
        return 2 * jnp.where(above < chips, above, chips - 2 - far) + flip

    for other in reversed(range(n - 1)):
        @pl.when(other < me)
        def _():
            copy(old, used, send_old, recv_old, other).start()

    speed = [speeds[node, pl.ds(0, rows), :] for node in range(3)]
    x0 = old[me, pl.ds(0, rows), :]
    half_step = 0.5 * slice_length

    def moved(weights):
        return slice_length * (weights[0] * speed[0] + weights[1] * speed[1] + weights[2] * speed[2])

    x1 = x0 + half_step * (speed[0] - speed[0]) + moved(lobatto_weights[0])
    first[me, pl.ds(0, rows), :] = x1

    def meet(other):
        pl.semaphore_wait(arrive.at[other], 1)
        copy(old, used, send_old, recv_old, other).start()

    def lanes_of(half):
        return pl.ds(half * LANES, LANES)

    def widen(node, ref, offset):
        for comp in range(3):
            for half in range(halves):
                line = ref[me, pl.ds(offset + comp * halves + half, 1), :]
                wide[node, comp, lanes_of(half), :] = jnp.broadcast_to(line, (LANES, LANES)).T

    def pairs(whose, parts, fresh):
        def one_chunk(index, carry):
            for node, ref, offset in parts:
                for part in range(chunk // 16):
                    span = pl.ds(pl.multiple_of(index * chunk, chunk) + part * 16, 16)
                    here = [wide[node, comp, span, :] for comp in range(3)]
                    sums = [None] * 3 if fresh else [total[node, comp, span, :] for comp in range(3)]
                    for half in range(halves):
                        gap = [ref[whose, pl.ds(offset + comp * halves + half, 1), :] - here[comp] for comp in range(3)]
                        weight = old[whose, pl.ds(weigh + half, 1), :]
                        squared = gap[0] * gap[0] + gap[1] * gap[1] + gap[2] * gap[2]
                        inverse = lax.rsqrt(squared + soften)
                        pull = (inverse * inverse) * (inverse * weight)
                        sums = [pull * gap[comp] if sums[comp] is None else sums[comp] + pull * gap[comp] for comp in range(3)]
                    for comp in range(3):
                        total[node, comp, span, :] = sums[comp]
            return carry

        lax.fori_loop(0, block // chunk, one_chunk, 0)

    ones = jnp.ones((8, 2 * LANES), jnp.bfloat16)

    def folded(comps):
        parts = []
        for comp in range(3):
            for half in range(halves):
                turned = comps[comp][half * LANES:(half + 1) * LANES, :].T
                parts.append(jnp.sum(turned, axis=0, keepdims=True))
        return jnp.concatenate(parts, axis=0) / body_count

    def added(node):
        return [total[node, comp] for comp in range(3)]

    old_parts = [(node, old, base[node]) for node in range(3)]

    def use_old(whose, fresh):
        pairs(whose, old_parts, fresh)

    def use_new(node, ref, whose, fresh):
        if fresh:
            widen(node, ref, 0)
        pairs(whose, [(node, ref, 0)], fresh)

    for node in range(3):
        widen(node, old, base[node])
    near = 2 * chip + 4
    for other in range(1, n):
        @pl.when((other > me) & (other < near))
        def _():
            meet(other)

    use_old(me, True)
    for other in range(1, n):
        @pl.when((other > me) & (other >= near))
        def _():
            meet(other)

    for index in range(n - 1):
        copy(first, rows, send_first, recv_first, seq(index)).start()

    @pl.when(me == leader)
    def _():
        pl.semaphore_wait(barrier, slices - 1)
        for step in range(1, slices):
            pl.semaphore_signal(ready, inc=1, device_id={"tm": (slot + step) % slices}, device_id_type=MESH)


    def with_old(step, carry):
        use_old(arrival(old, used, send_old, recv_old, step), False)
        return carry

    lax.fori_loop(1, n, with_old, 0)

    def kicked(weights, drop):
        parts = [weights[node] * slice_length for node in range(3)]
        parts[1] = parts[1] - drop
        return folded([parts[0] * total[0, comp] + parts[1] * total[1, comp] + parts[2] * total[2, comp] for comp in range(3)])

    v0 = speed[0]
    v1 = v0 + kicked(lobatto_weights[0], 0.0)
    x2 = x1 + half_step * (v1 - speed[1]) + moved(lobatto_weights[1])
    last[me, pl.ds(0, rows), :] = x2
    for index in range(n - 1):
        copy(last, rows, send_last, recv_last, up(index)).start()

    @pl.when(me == leader)
    def _():
        pl.semaphore_wait(ready, slices - 1)
        for other in range(n):
            if other != leader:
                pl.semaphore_signal(go, inc=1, device_id={"space": other}, device_id_type=MESH)

    kick = kicked(lobatto_weights[1], half_step)
    use_new(3, first, me, True)

    def only_first(step, carry):
        use_new(3, first, arrival(first, rows, send_first, recv_first, step), False)
        return carry

    lax.fori_loop(1, n, only_first, 0)
    a1 = folded(added(3))
    v2 = v1 + half_step * a1 + kick
    drift_rows = drift.shape[1] // 2
    drift[slot, pl.ds(0, rows), :] = x2 - (x0 + slice_length * v0)
    drift[slot, pl.ds(drift_rows, rows), :] = v2 - v0

    def drift_copy(step, whose, to):
        return pltpu.make_async_remote_copy(
            src_ref=drift.at[whose], dst_ref=drift.at[whose], send_sem=send_drift.at[step], recv_sem=recv_drift.at[step],
            device_id={"tm": to}, device_id_type=MESH,
        )

    @pl.when(me != leader)
    def _():
        pl.semaphore_wait(go, 1)

    for step in range(1, slices):
        @pl.when(slot + step < slices)
        def _():
            drift_copy(step, slot, slot + step).start()

    use_new(4, last, me, True)

    def put(ref, value):
        for row in range(rows):
            ref[row] = value[row:row + 1, :]

    def put_pair(ref, value1, value2):
        for comp in range(3):
            for half in range(halves):
                row = comp * halves + half
                ref[comp, half, 0:1, :] = value1[row:row + 1, :]
                ref[comp, half, 1:2, :] = value2[row:row + 1, :]

    put_pair(places_out, x1, x2)
    put_pair(speeds_out, v1, v2)

    def in_rows(value):
        return jnp.concatenate(
            [value[comp:comp + 1, half * LANES:(half + 1) * LANES] for comp in range(3) for half in range(halves)], axis=0
        )

    start_speed = in_rows(own[1])
    put(start_speed_out, start_speed)
    put(start_out, in_rows(own[0]) + slot.astype(f32) * slice_length * start_speed)

    for step in range(1, n):
        copy(old, used, send_old, recv_old, target_of(me, step, n)).wait_send()
        copy(first, rows, send_first, recv_first, target_of(me, step, n)).wait_send()

    for step in range(1, n):
        copy(last, rows, send_last, recv_last, target_of(me, step, n)).wait_send()

    def only_last(step, carry):
        use_new(4, last, arrival(last, rows, send_last, recv_last, step), False)
        return carry

    lax.fori_loop(1, n, only_last, 0)
    put(force_out, folded(added(4)))

    for step in range(1, slices):
        @pl.when(slot >= step)
        def _():
            whose = slot - step
            drift_copy(step, whose, whose).wait_recv()
            moved_place = drift[whose, pl.ds(0, rows), :]
            moved_speed = drift[whose, pl.ds(drift_rows, rows), :]
            ahead = moved_place + ((step - 1) * slice_length) * moved_speed
            for row in range(rows):
                start_out[row] = start_out[row] + ahead[row:row + 1, :]
                start_speed_out[row] = start_speed_out[row] + moved_speed[row:row + 1, :]

    for step in range(1, slices):
        @pl.when(slot + step < slices)
        def _():
            drift_copy(step, slot, slot + step).wait_send()


def write_out(*refs):
    copies = [pltpu.make_async_copy(refs[i], refs[5 + i], refs[10].at[i]) for i in range(5)]
    for copy in copies:
        copy.start()
    for copy in copies:
        copy.wait()


def solution(mesh):
    n, slices = mesh.shape["space"], mesh.shape["tm"]

    def body(positions, velocities, masses, initial_places, initial_speeds):
        block = positions.shape[3]
        halves = block // LANES
        stack = round_up(10 * halves, 8)
        part = round_up(3 * halves, 8)
        f32 = jnp.float32
        vmem = pl.BlockSpec(memory_space=pltpu.VMEM)
        dma = pltpu.SemaphoreType.DMA
        rows = 3 * halves
        shapes = [(3, halves, 2, LANES)] * 2 + [(rows, 1, LANES)] * 3
        anywhere = pl.BlockSpec(memory_space=pl.ANY)
        outs = pl.pallas_call(
            functools.partial(kernel, n, slices, float(block * n), block),
            out_shape=tuple(pltpu.VMEM(shape, f32) for shape in shapes),
            in_specs=[anywhere] * 5,
            out_specs=(vmem,) * 5,
            scratch_shapes=[
                pltpu.VMEM((n, stack, LANES), f32),
                pltpu.VMEM((n, part, LANES), f32),
                pltpu.VMEM((n, part, LANES), f32),
                pltpu.VMEM((slices, 2 * part, LANES), f32),
                pltpu.VMEM((3, part, LANES), f32),
                pltpu.VMEM((2, 3, block), f32),
                dma((9,)),
                pltpu.VMEM((5, 3, block, LANES), f32),
                pltpu.VMEM((5, 3, block, LANES), f32),
                dma((n,)), dma((n,)), dma((n,)), dma((n,)), dma((n,)), dma((n,)),
                dma((slices,)), dma((slices,)),
                pltpu.SemaphoreType.REGULAR, pltpu.SemaphoreType.REGULAR, pltpu.SemaphoreType.REGULAR((n,)),
            ],
            compiler_params=pltpu.CompilerParams(collective_id=0, has_side_effects=True),
        )(
            positions.reshape(3 * rows, 1, LANES),
            velocities.reshape(3 * rows, 1, LANES),
            masses.reshape(halves, 1, LANES),
            initial_places,
            initial_speeds,
        )
        outs = pl.pallas_call(
            write_out,
            out_shape=tuple(jax.ShapeDtypeStruct(shape, f32) for shape in shapes),
            in_specs=[vmem] * 5,
            out_specs=(anywhere,) * 5,
            scratch_shapes=[dma((5,))],
        )(*(pltpu.with_memory_space_constraint(part, pltpu.VMEM) for part in outs))
        paired = [part.transpose(2, 0, 1, 3).reshape(1, 2, 3, block) for part in outs[:2]]
        return (*paired, *(part.reshape(1, 3, block) for part in outs[2:]))

    return jax.shard_map(
        body,
        mesh=mesh,
        in_specs=(
            P("tm", None, None, "space"),
            P("tm", None, None, "space"),
            P("space"),
            P(None, "space"),
            P(None, "space"),
        ),
        out_specs=(
            P("tm", None, None, "space"),
            P("tm", None, None, "space"),
            P("tm", None, "space"),
            P("tm", None, "space"),
            P("tm", None, "space"),
        ),
        check_vma=False,
    )
```

```python
import functools
import jax
import jax.numpy as jnp
from jax import lax
from jax.experimental import pallas as pl
from jax.experimental.pallas import tpu as pltpu
from jax.sharding import PartitionSpec as P

soften = 0.01
slice_length = 0.25
lobatto_weights = ((5.0 / 24.0, 1.0 / 3.0, -1.0 / 24.0), (-1.0 / 24.0, 1.0 / 3.0, 5.0 / 24.0))
LANES = 128
MESH = pl.DeviceIdType.MESH


def round_up(value, step):
    return (value + step - 1) // step * step


def target_of(me, step, count):
    if count & (count - 1) == 0:
        peer, bit = 0, 1
        while bit < count:
            peer = peer + ((me // bit + step // bit) % 2) * bit
            bit *= 2
        return peer
    return (me + step) % count


def source_of(me, step, count):
    if count & (count - 1) == 0:
        return target_of(me, step, count)
    return (me + count - step) % count


def kernel(
    n, slices, body_count, chunk,
    pos, vel, mass, place0, speed0,
    places_out, speeds_out, force_out, start_out, start_speed_out,
    old, first, last, drift, speeds, own, load_sem, wide, total,
    send_old, recv_old, send_first, recv_first, send_last, recv_last, send_drift, recv_drift, ready, go, arrive,
):
    me = lax.axis_index("space")
    slot = lax.axis_index("tm")
    halves = mass.shape[0]
    block = halves * LANES
    rows = 3 * halves
    weigh = rows
    base = (0, rows + halves, 2 * rows + halves)
    used = 3 * rows + halves
    f32 = jnp.float32

    loads = [
        pltpu.make_async_copy(mass.at[:, 0, :], old.at[me, pl.ds(weigh, halves), :], load_sem.at[0]),
        pltpu.make_async_copy(place0, own.at[0], load_sem.at[1]),
        pltpu.make_async_copy(speed0, own.at[1], load_sem.at[2]),
    ]
    for node in range(3):
        span = pl.ds(node * rows, rows)
        loads.append(pltpu.make_async_copy(pos.at[span, 0, :], old.at[me, pl.ds(base[node], rows), :], load_sem.at[3 + node]))
        loads.append(pltpu.make_async_copy(vel.at[span, 0, :], speeds.at[node, pl.ds(0, rows), :], load_sem.at[6 + node]))
    for load in loads:
        load.start()

    leader = 0
    barrier = pltpu.get_barrier_semaphore()
    for other in range(1, n):
        @pl.when(other > me)
        def _():
            pl.semaphore_signal(barrier, inc=1, device_id={"space": other}, device_id_type=MESH)

    @pl.when(me == leader)
    def _():
        for step in range(1, slices):
            pl.semaphore_signal(barrier, inc=1, device_id={"tm": (slot + step) % slices}, device_id_type=MESH)

    @pl.when(me > 0)
    def _():
        pl.semaphore_wait(barrier, me)

    for other in reversed(range(n - 1)):
        @pl.when(other < me)
        def _():
            pl.semaphore_signal(arrive.at[me], inc=1, device_id={"space": other}, device_id_type=MESH)

    for load in loads:
        load.wait()

    chips = n // 2
    chip, core = me // 2, me % 2

    def copy(ref, count, send, recv, to):
        span = pl.ds(0, count)
        return pltpu.make_async_remote_copy(
            src_ref=ref.at[me, span, :], dst_ref=ref.at[me, span, :], send_sem=send.at[to], recv_sem=recv.at[me],
            device_id={"space": to}, device_id_type=MESH,
        )

    def whose_at(step):
        far = (step - 2) // 2
        side = (step - 2) % 2
        flip = core + side - 2 * core * side
        other = 2 * jnp.where(far < chip, chip - 1 - far, far + 1) + flip
        return jnp.where(step == 1, me + 1 - 2 * core, other)

    def arrival(ref, count, send, recv, step):
        whose = whose_at(step)
        span = pl.ds(0, count)
        pltpu.make_async_remote_copy(
            src_ref=ref.at[whose, span, :], dst_ref=ref.at[whose, span, :], send_sem=send.at[whose], recv_sem=recv.at[whose],
            device_id={"space": whose}, device_id_type=MESH,
        ).wait_recv()
        return whose

    def up(index):
        return index + jnp.where(index < me, 0, 1)

    def seq(index):
        if index == 0:
            return me + 1 - 2 * core
        far, side = (index - 1) // 2, (index - 1) % 2
        above = chip + 1 + far
        flip = core + side - 2 * core * side
        return 2 * jnp.where(above < chips, above, chips - 2 - far) + flip

    for other in reversed(range(n - 1)):
        @pl.when(other < me)
        def _():
            copy(old, used, send_old, recv_old, other).start()

    speed = [speeds[node, pl.ds(0, rows), :] for node in range(3)]
    x0 = old[me, pl.ds(0, rows), :]
    half_step = 0.5 * slice_length

    def moved(weights):
        return slice_length * (weights[0] * speed[0] + weights[1] * speed[1] + weights[2] * speed[2])

    x1 = x0 + half_step * (speed[0] - speed[0]) + moved(lobatto_weights[0])
    first[me, pl.ds(0, rows), :] = x1

    def meet(other):
        pl.semaphore_wait(arrive.at[other], 1)
        copy(old, used, send_old, recv_old, other).start()

    def lanes_of(half):
        return pl.ds(half * LANES, LANES)

    def widen(node, ref, offset):
        for comp in range(3):
            for half in range(halves):
                line = ref[me, pl.ds(offset + comp * halves + half, 1), :]
                wide[node, comp, lanes_of(half), :] = jnp.broadcast_to(line, (LANES, LANES)).T

    def pairs(whose, parts, fresh):
        def one_chunk(index, carry):
            for node, ref, offset in parts:
                for part in range(chunk // 16):
                    span = pl.ds(pl.multiple_of(index * chunk, chunk) + part * 16, 16)
                    here = [wide[node, comp, span, :] for comp in range(3)]
                    sums = [None] * 3 if fresh else [total[node, comp, span, :] for comp in range(3)]
                    for half in range(halves):
                        gap = [ref[whose, pl.ds(offset + comp * halves + half, 1), :] - here[comp] for comp in range(3)]
                        weight = old[whose, pl.ds(weigh + half, 1), :]
                        squared = gap[0] * gap[0] + gap[1] * gap[1] + gap[2] * gap[2]
                        inverse = lax.rsqrt(squared + soften)
                        pull = (inverse * inverse) * (inverse * weight)
                        sums = [pull * gap[comp] if sums[comp] is None else sums[comp] + pull * gap[comp] for comp in range(3)]
                    for comp in range(3):
                        total[node, comp, span, :] = sums[comp]
            return carry

        lax.fori_loop(0, block // chunk, one_chunk, 0)

    ones = jnp.ones((8, 2 * LANES), jnp.bfloat16)

    def folded(comps):
        parts = []
        for comp in range(3):
            for half in range(halves):
                turned = comps[comp][half * LANES:(half + 1) * LANES, :].T
                parts.append(jnp.sum(turned, axis=0, keepdims=True))
        return jnp.concatenate(parts, axis=0) * (1.0 / body_count)

    def added(node):
        return [total[node, comp] for comp in range(3)]

    old_parts = [(node, old, base[node]) for node in range(3)]

    def use_old(whose, fresh):
        pairs(whose, old_parts, fresh)

    def use_new(node, ref, whose, fresh):
        if fresh:
            widen(node, ref, 0)
        pairs(whose, [(node, ref, 0)], fresh)

    for node in range(3):
        widen(node, old, base[node])
    near = 2 * chip + 4
    for other in range(1, n):
        @pl.when((other > me) & (other < near))
        def _():
            meet(other)

    use_old(me, True)
    for other in range(1, n):
        @pl.when((other > me) & (other >= near))
        def _():
            meet(other)

    for index in range(n - 1):
        copy(first, rows, send_first, recv_first, seq(index)).start()

    @pl.when(me == leader)
    def _():
        pl.semaphore_wait(barrier, slices - 1)
        for step in range(1, slices):
            pl.semaphore_signal(ready, inc=1, device_id={"tm": (slot + step) % slices}, device_id_type=MESH)


    def with_old(step, carry):
        use_old(arrival(old, used, send_old, recv_old, step), False)
        return carry

    lax.fori_loop(1, n, with_old, 0)

    def kicked(weights, drop):
        parts = [weights[node] * slice_length for node in range(3)]
        parts[1] = parts[1] - drop
        return folded([parts[0] * total[0, comp] + parts[1] * total[1, comp] + parts[2] * total[2, comp] for comp in range(3)])

    v0 = speed[0]
    v1 = v0 + kicked(lobatto_weights[0], 0.0)
    x2 = x1 + half_step * (v1 - speed[1]) + moved(lobatto_weights[1])
    last[me, pl.ds(0, rows), :] = x2
    for index in range(n - 1):
        copy(last, rows, send_last, recv_last, up(index)).start()

    @pl.when(me == leader)
    def _():
        pl.semaphore_wait(ready, slices - 1)
        for other in range(n):
            if other != leader:
                pl.semaphore_signal(go, inc=1, device_id={"space": other}, device_id_type=MESH)

    kick = kicked(lobatto_weights[1], half_step)
    use_new(3, first, me, True)

    def only_first(step, carry):
        use_new(3, first, arrival(first, rows, send_first, recv_first, step), False)
        return carry

    lax.fori_loop(1, n, only_first, 0)
    a1 = folded(added(3))
    v2 = v1 + half_step * a1 + kick
    drift_rows = drift.shape[1] // 2
    drift[slot, pl.ds(0, rows), :] = x2 - (x0 + slice_length * v0)
    drift[slot, pl.ds(drift_rows, rows), :] = v2 - v0

    def drift_copy(step, whose, to):
        return pltpu.make_async_remote_copy(
            src_ref=drift.at[whose], dst_ref=drift.at[whose], send_sem=send_drift.at[step], recv_sem=recv_drift.at[step],
            device_id={"tm": to}, device_id_type=MESH,
        )

    @pl.when(me != leader)
    def _():
        pl.semaphore_wait(go, 1)

    for step in range(1, slices):
        @pl.when(slot + step < slices)
        def _():
            drift_copy(step, slot, slot + step).start()

    use_new(4, last, me, True)

    def put(ref, value):
        for row in range(rows):
            ref[row] = value[row:row + 1, :]

    def put_pair(ref, value1, value2):
        for comp in range(3):
            for half in range(halves):
                row = comp * halves + half
                ref[comp, half, 0:1, :] = value1[row:row + 1, :]
                ref[comp, half, 1:2, :] = value2[row:row + 1, :]

    put_pair(places_out, x1, x2)
    put_pair(speeds_out, v1, v2)

    def in_rows(value):
        return jnp.concatenate(
            [value[comp:comp + 1, half * LANES:(half + 1) * LANES] for comp in range(3) for half in range(halves)], axis=0
        )

    start_speed = in_rows(own[1])
    put(start_speed_out, start_speed)
    put(start_out, in_rows(own[0]) + slot.astype(f32) * slice_length * start_speed)

    for step in range(1, n):
        copy(old, used, send_old, recv_old, target_of(me, step, n)).wait_send()
        copy(first, rows, send_first, recv_first, target_of(me, step, n)).wait_send()

    for step in range(1, n):
        copy(last, rows, send_last, recv_last, target_of(me, step, n)).wait_send()

    def only_last(step, carry):
        use_new(4, last, arrival(last, rows, send_last, recv_last, step), False)
        return carry

    lax.fori_loop(1, n, only_last, 0)
    put(force_out, folded(added(4)))

    for step in range(1, slices):
        @pl.when(slot >= step)
        def _():
            whose = slot - step
            drift_copy(step, whose, whose).wait_recv()
            moved_place = drift[whose, pl.ds(0, rows), :]
            moved_speed = drift[whose, pl.ds(drift_rows, rows), :]
            ahead = moved_place + ((step - 1) * slice_length) * moved_speed
            for row in range(rows):
                start_out[row] = start_out[row] + ahead[row:row + 1, :]
                start_speed_out[row] = start_speed_out[row] + moved_speed[row:row + 1, :]

    for step in range(1, slices):
        @pl.when(slot + step < slices)
        def _():
            drift_copy(step, slot, slot + step).wait_send()


def write_out(*refs):
    copies = [pltpu.make_async_copy(refs[i], refs[5 + i], refs[10].at[i]) for i in range(5)]
    for copy in copies:
        copy.start()
    for copy in copies:
        copy.wait()


def solution(mesh):
    n, slices = mesh.shape["space"], mesh.shape["tm"]

    def body(positions, velocities, masses, initial_places, initial_speeds):
        block = positions.shape[3]
        halves = block // LANES
        stack = round_up(10 * halves, 8)
        part = round_up(3 * halves, 8)
        f32 = jnp.float32
        vmem = pl.BlockSpec(memory_space=pltpu.VMEM)
        dma = pltpu.SemaphoreType.DMA
        rows = 3 * halves
        shapes = [(3, halves, 2, LANES)] * 2 + [(rows, 1, LANES)] * 3
        anywhere = pl.BlockSpec(memory_space=pl.ANY)
        outs = pl.pallas_call(
            functools.partial(kernel, n, slices, float(block * n), block),
            out_shape=tuple(pltpu.VMEM(shape, f32) for shape in shapes),
            in_specs=[anywhere] * 5,
            out_specs=(vmem,) * 5,
            scratch_shapes=[
                pltpu.VMEM((n, stack, LANES), f32),
                pltpu.VMEM((n, part, LANES), f32),
                pltpu.VMEM((n, part, LANES), f32),
                pltpu.VMEM((slices, 2 * part, LANES), f32),
                pltpu.VMEM((3, part, LANES), f32),
                pltpu.VMEM((2, 3, block), f32),
                dma((9,)),
                pltpu.VMEM((5, 3, block, LANES), f32),
                pltpu.VMEM((5, 3, block, LANES), f32),
                dma((n,)), dma((n,)), dma((n,)), dma((n,)), dma((n,)), dma((n,)),
                dma((slices,)), dma((slices,)),
                pltpu.SemaphoreType.REGULAR, pltpu.SemaphoreType.REGULAR, pltpu.SemaphoreType.REGULAR((n,)),
            ],
            compiler_params=pltpu.CompilerParams(collective_id=0, has_side_effects=True),
        )(
            positions.reshape(3 * rows, 1, LANES),
            velocities.reshape(3 * rows, 1, LANES),
            masses.reshape(halves, 1, LANES),
            initial_places,
            initial_speeds,
        )
        outs = pl.pallas_call(
            write_out,
            out_shape=tuple(jax.ShapeDtypeStruct(shape, f32) for shape in shapes),
            in_specs=[vmem] * 5,
            out_specs=(anywhere,) * 5,
            scratch_shapes=[dma((5,))],
        )(*(pltpu.with_memory_space_constraint(part, pltpu.VMEM) for part in outs))
        paired = [part.transpose(2, 0, 1, 3).reshape(1, 2, 3, block) for part in outs[:2]]
        return (*paired, *(part.reshape(1, 3, block) for part in outs[2:]))

    return jax.shard_map(
        body,
        mesh=mesh,
        in_specs=(
            P("tm", None, None, "space"),
            P("tm", None, None, "space"),
            P("space"),
            P(None, "space"),
            P(None, "space"),
        ),
        out_specs=(
            P("tm", None, None, "space"),
            P("tm", None, None, "space"),
            P("tm", None, "space"),
            P("tm", None, "space"),
            P("tm", None, "space"),
        ),
        check_vma=False,
    )
```
